32 devices in a mesh: seq: 8 (over z, core), head: 4 (over y, x).
Axes of the slice: x: 2, y: 2, z: 4, core: 2. Of those that a mesh axis runs over, the one named last changes fastest.
Arguments:
- queries: bfloat16 [1024, 128, 576], P('seq', 'head'), may hold values from -24 to 24
- latent_kv: bfloat16 [1024, 576], P('seq'), may hold values from -4.5 to 4.5
- grad_out: bfloat16 [1024, 128, 512], P('seq', 'head'), may hold values from -6 to 6
- doc_start: int32 [1024], P('seq'), may hold values from 0 to 1023, as said below
Outputs:
- grad_queries: bfloat16 [1024, 128, 576], P('seq', 'head')
- grad_latent: float32 [1024, 576], P('seq')
The draws below stay inside these ranges and needn't reach their ends.
Inputs may be any that keep to these rules, and one draw needn't show every extreme that they name: doc_start[p] is the first position of the document holding position p: it never falls along the sequence, doc_start[p] <= p, doc_start[0] = 0, every document holds at most 385 positions, and one document holds exactly 385.
All inputs are finite; a program needn't handle non-finite values.
Results may differ from the reference program's by a relative error of at most 0.0048.
Values may be sent and summed in bfloat16 or wider, within the bound.
A program may use at most 128 MiB of HBM per device.

```python
import jax
import jax.numpy as jnp
from jax import lax

HEADS = 128
LAT = 512
KVW = 576
TOK_DEV = 128
REACH = 4
DOC_MAX = 385
SEQ_LEN = 1024
N_SEQ = 8


def document_starts(key):
    places = jnp.arange(SEQ_LEN, dtype=jnp.int32)
    lengths = jax.random.randint(jax.random.fold_in(key, 11), (SEQ_LEN,), 1, DOC_MAX + 1)
    chosen_doc = jax.random.randint(jax.random.fold_in(key, 12), (), 0, 2)
    lengths = jnp.where(places == chosen_doc, DOC_MAX, lengths)
    begins = jnp.cumsum(lengths) - lengths
    marks = jnp.zeros((SEQ_LEN,), jnp.int32).at[begins].max(1, mode='drop')
    start_marks = jnp.where((marks == 1) | (places == 0), places, 0)
    return lax.cummax(start_marks, axis=0)


def latent_base(key):
    return jnp.clip(jax.random.normal(jax.random.fold_in(key, 21), (SEQ_LEN, KVW), jnp.float32), -4.0, 4.0)


def draw_doc_start(key, part):
    return document_starts(key)


def draw_latent_kv(key, part):
    latent = latent_base(key)
    return latent.astype(jnp.bfloat16)


def draw_queries(key, part):
    gaussian = jax.random.normal(jax.random.fold_in(key, 31), (SEQ_LEN, HEADS, KVW), jnp.float32)
    return (0.4 * jnp.clip(gaussian, -6.0, 6.0)).astype(jnp.bfloat16)


def levels(stream_key, shape, cuts, low, high):
    gain = 1.0
    for dim, blocks in cuts:
        draws = jax.random.uniform(jax.random.fold_in(jax.random.fold_in(stream_key, 6), dim), (blocks,), jnp.float32, low / len(cuts), high / len(cuts))
        gain = gain * jnp.repeat(jnp.exp(draws), shape[dim] // blocks).reshape((-1,) + (1,) * (len(shape) - 1 - dim))
    return gain


def scatter_about(key, dims, deviation, reach, cuts=(), held_as=jnp.bfloat16):
    array = jax.random.normal(key, dims, jnp.float32) * deviation
    if len(cuts) > 0:
        array = levels(key, dims, cuts, -0.22, 0.18) * array
    return jnp.clip(array, min=-reach, max=reach).astype(held_as)


def setup_inputs(seed: int = 0) -> dict:
    splits = jax.random.split(jax.random.key(seed), 5)
    queries = draw_queries(jax.random.fold_in(splits[4], 71), 0)
    latent_kv = draw_latent_kv(jax.random.fold_in(splits[4], 71), 0)
    grad_out = scatter_about(splits[2], (SEQ_LEN, HEADS, LAT), 1.0, 6.0, ((0, 8), (1, 4)))
    doc_start = draw_doc_start(jax.random.fold_in(splits[4], 71), 0)
    return dict(queries=queries, latent_kv=latent_kv, grad_out=grad_out, doc_start=doc_start)


softmax_scale = 192.0 ** -0.5
lowest = -1.0e30
contract_first = (((0,), (0,)), ((), ()))
contract_last = (((1,), (1,)), ((), ()))


def reference(queries, latent_kv, grad_out, doc_start):
    margin = (REACH - 1) * TOK_DEV
    window = REACH * TOK_DEV
    kv_padded = jnp.concatenate([jnp.zeros((margin, KVW), jnp.bfloat16), latent_kv], axis=0)
    grad_padded = jnp.zeros((SEQ_LEN + margin, KVW), jnp.float32)

    def one_block(grad_pad, block_index):
        first = block_index * TOK_DEV
        query_rows = lax.dynamic_slice_in_dim(queries, first, TOK_DEV, 0).reshape(TOK_DEV * HEADS, KVW)
        grad_rows = lax.dynamic_slice_in_dim(grad_out, first, TOK_DEV, 0).reshape(TOK_DEV * HEADS, LAT)
        kv_block = lax.dynamic_slice_in_dim(kv_padded, first, window, 0)
        row_pos = jnp.repeat(first + jnp.arange(TOK_DEV, dtype=jnp.int32), HEADS)
        row_first = jnp.repeat(lax.dynamic_slice_in_dim(doc_start, first, TOK_DEV, 0), HEADS)
        key_pos = first - margin + jnp.arange(window, dtype=jnp.int32)
        visible = (key_pos[None, :] <= row_pos[:, None]) & (key_pos[None, :] >= row_first[:, None])
        scores = lax.dot_general(query_rows, kv_block, contract_last, preferred_element_type=jnp.float32) * softmax_scale
        row_top = jnp.max(jnp.where(visible, scores, lowest), axis=1)
        total_exp = jnp.sum(jnp.where(visible, jnp.exp(scores - row_top[:, None]), 0.0), axis=1)
        log_total = row_top + jnp.log(total_exp)
        probs = jnp.where(visible, jnp.exp(scores - log_total[:, None]), 0.0)
        grad_probs = lax.dot_general(grad_rows, kv_block[:, :LAT], contract_last, preferred_element_type=jnp.float32)
        delta = jnp.sum(probs * grad_probs, axis=1)
        grad_scores = (probs * (grad_probs - delta[:, None])).astype(jnp.bfloat16)
        probs_bf = probs.astype(jnp.bfloat16)
        grad_query = (jnp.dot(grad_scores, kv_block, preferred_element_type=jnp.float32) * softmax_scale).astype(jnp.bfloat16)
        from_scores = lax.dot_general(grad_scores, query_rows, contract_first, preferred_element_type=jnp.float32) * softmax_scale
        from_values = lax.dot_general(probs_bf, grad_rows, contract_first, preferred_element_type=jnp.float32)
        term = jnp.concatenate([from_scores[:, :LAT] + from_values, from_scores[:, LAT:]], axis=1)
        old = lax.dynamic_slice_in_dim(grad_pad, first, window, 0)
        grad_pad = lax.dynamic_update_slice_in_dim(grad_pad, old + term, first, 0)
        return grad_pad, grad_query.reshape(TOK_DEV, HEADS, KVW)

    grad_padded, grad_blocks = lax.scan(one_block, grad_padded, jnp.arange(N_SEQ, dtype=jnp.int32))
    grad_queries = grad_blocks.reshape(SEQ_LEN, HEADS, KVW)
    return (grad_queries, grad_padded[margin:])
```

```python
import math
from functools import partial

import jax
import jax.numpy as jnp
from jax import lax
from jax.experimental import pallas as pl
from jax.experimental.pallas import tpu as pltpu
from jax.sharding import PartitionSpec as P

LAT = 512
REACH = 4


softmax_scale = 192.0 ** (-0.5)
lowest = -1e30
contract_last = (((1,), (1,)), ((), ()))
contract_first = (((0,), (0,)), ((), ()))


def passed_along(block, axis, distance):
    devices = range(lax.axis_size(axis))
    route = [(i - distance, i) for i in devices if i - distance in devices]
    return lax.ppermute(block, axis, route)


def product_tiles(query_rows, grad_rows, kv_block, unused):
    scores = (
        lax.dot_general(query_rows, kv_block, contract_last, preferred_element_type=jnp.float32)
        * softmax_scale
    )
    grad_probs = lax.dot_general(
        grad_rows, kv_block[:, :LAT], contract_last, preferred_element_type=jnp.float32
    )
    return (scores, grad_probs)


def empty_tiles(query_count, key_count, unused):
    blank = jnp.zeros((query_count, key_count), jnp.float32)
    return (blank, blank)


def grads_update(
    query_rows, grad_rows, kv_block, scores, grad_probs, visible, log_total, row_delta, unused
):
    weights = jnp.where(visible, jnp.exp(scores - log_total[:, None]), 0.0)
    grad_bf = (weights * (grad_probs - row_delta[:, None])).astype(jnp.bfloat16)
    prob_bf = weights.astype(jnp.bfloat16)
    query_part = jnp.dot(grad_bf, kv_block, preferred_element_type=jnp.float32)
    from_scores = (
        lax.dot_general(grad_bf, query_rows, contract_first, preferred_element_type=jnp.float32)
        * softmax_scale
    )
    from_values = lax.dot_general(
        prob_bf, grad_rows, contract_first, preferred_element_type=jnp.float32
    )
    term = jnp.concatenate([from_scores[:, :LAT] + from_values, from_scores[:, LAT:]], axis=1)
    return (query_part, term)


def no_grads(query_count, tokens, row_width, unused):
    return (
        jnp.zeros((query_count, row_width), jnp.float32),
        jnp.zeros((tokens, row_width), jnp.float32),
    )


def per_device(queries, latent_kv, grad_out, doc_start):
    tokens, head_local, row_width = queries.shape
    query_count = tokens * head_local
    first_pos = lax.axis_index("seq") * tokens
    query_rows = queries.reshape(query_count, row_width)
    grad_rows = grad_out.reshape(query_count, LAT)
    row_pos = jnp.repeat(first_pos + jnp.arange(tokens, dtype=jnp.int32), head_local)
    row_first = jnp.repeat(doc_start, head_local)
    low_first = jnp.min(doc_start)
    windows = [latent_kv]
    for distance in range(1, REACH):
        windows.append(passed_along(latent_kv, "seq", distance))
    key_starts = [first_pos - distance * tokens for distance in range(REACH)]
    wanted = [start + tokens > low_first for start in key_starts]
    blank = jnp.zeros((query_count,), jnp.float32)
    row_top = jnp.full((query_count,), lowest, jnp.float32)
    total_exp = blank
    weighted = blank
    kept = []
    for distance in range(REACH):
        scores, grad_probs = lax.cond(
            wanted[distance],
            partial(product_tiles, query_rows, grad_rows, windows[distance]),
            partial(empty_tiles, query_count, tokens),
            0,
        )
        key_pos = key_starts[distance] + jnp.arange(tokens, dtype=jnp.int32)
        visible = (key_pos[None, :] <= row_pos[:, None]) & (key_pos[None, :] >= row_first[:, None])
        new_top = jnp.maximum(row_top, jnp.max(jnp.where(visible, scores, lowest), axis=1))
        rescale = jnp.exp(row_top - new_top)
        weights = jnp.where(visible, jnp.exp(scores - new_top[:, None]), 0.0)
        total_exp = total_exp * rescale + jnp.sum(weights, axis=1)
        weighted = weighted * rescale + jnp.sum(weights * grad_probs, axis=1)
        row_top = new_top
        kept.append((scores, grad_probs, visible))
    log_total = row_top + jnp.log(total_exp)
    row_delta = weighted / total_exp
    query_grad = jnp.zeros((query_count, row_width), jnp.float32)
    terms = []
    for distance in range(REACH):
        scores, grad_probs, visible = kept[distance]
        compute = partial(
            grads_update,
            query_rows,
            grad_rows,
            windows[distance],
            scores,
            grad_probs,
            visible,
            log_total,
            row_delta,
        )
        query_part, term = lax.cond(
            wanted[distance], compute, partial(no_grads, query_count, tokens, row_width), 0
        )
        query_grad = query_grad + query_part
        terms.append(term)
    own_rows = terms[0]
    for distance in range(1, REACH):
        own_rows = own_rows + passed_along(
            terms[distance].astype(jnp.bfloat16), "seq", -distance
        ).astype(jnp.float32)
    grad_latent = lax.psum(own_rows, "head")
    grad_queries = (
        (softmax_scale * query_grad).astype(jnp.bfloat16).reshape(tokens, head_local, row_width)
    )
    return (grad_queries, grad_latent)


TILE_HEADS = 4
MESH = pl.DeviceIdType.MESH


def fused_kernel(
    n_seq, n_head, head_local, tokens,
    q_hbm, g_hbm, kv_ref, first_ref,
    dq_hbm, out_ref,
    q, g, dq, ds, pb, win, win_t, bias, parts, *rest,
):
    cuts = parts
    n_cut = len(cuts)
    take = iter(rest)
    own = [next(take) for _ in range(n_cut)]
    t_send = [next(take) for _ in range(n_cut)]
    t_recv = [next(take) for _ in range(n_cut)]
    r_send = [next(take) for _ in range(n_cut)]
    r_recv = [next(take) for _ in range(n_cut)]
    r_own = [next(take) for _ in range(n_cut)]
    f_send = [next(take) for _ in range(n_cut)]
    f_recv = [next(take) for _ in range(n_cut)]
    (load_sem, q_sem, store_sem, g1s, g1r, g2s, g2r, r1s, r1r, r2s, r2r, r3s, r3r) = take

    s = lax.axis_index("seq")
    h = lax.axis_index("head")
    width = kv_ref.shape[1]
    quarter = tokens // n_head
    tile_rows = TILE_HEADS * tokens
    n_tile = head_local // TILE_HEADS
    margin = (REACH - 1) * tokens
    window = REACH * tokens
    peers = range(1, n_head)
    reach = range(1, REACH)

    def peer(k):
        return lax.rem(h + k, n_head)

    def load_q(i):
        lanes = pl.ds(pl.multiple_of(i * tokens, tokens), tokens)
        return pltpu.make_async_copy(q_hbm.at[i], q.at[:, lanes], q_sem.at[i])

    loads = [
        pltpu.make_async_copy(g_hbm, g, load_sem.at[0]),
        pltpu.make_async_copy(kv_ref, win.at[pl.ds(margin, tokens)], load_sem.at[1]),
    ]
    for copy in loads:
        copy.start()

    @pl.loop(0, head_local)
    def _(i):
        load_q(i).start()

    barrier = pltpu.get_barrier_semaphore()
    for k in peers:
        pl.semaphore_signal(barrier, inc=1, device_id=(s, peer(k)), device_id_type=MESH)
    for d in reach:
        @pl.when(s >= d)
        def _():
            pl.semaphore_signal(barrier, inc=1, device_id=(s - d, h), device_id_type=MESH)

        @pl.when(s + d < n_seq)
        def _():
            pl.semaphore_signal(barrier, inc=1, device_id=(s + d, h), device_id_type=MESH)

    before = jnp.minimum(s, REACH - 1)
    after = jnp.minimum(n_seq - 1 - s, REACH - 1)
    pl.semaphore_wait(barrier, n_head - 1 + before + after)

    share = pl.multiple_of(h * quarter, quarter)

    def along(d):
        return pltpu.make_async_remote_copy(
            src_ref=kv_ref.at[pl.ds(share, quarter)],
            dst_ref=win.at[pl.ds((REACH - 1 - d) * tokens + share, quarter)],
            send_sem=g1s.at[d - 1], recv_sem=g1r.at[d - 1],
            device_id=(s + d, h), device_id_type=MESH,
        )

    def across(d, k):
        rows = pl.ds((REACH - 1 - d) * tokens + share, quarter)
        return pltpu.make_async_remote_copy(
            src_ref=win.at[rows], dst_ref=win.at[rows],
            send_sem=g2s.at[d - 1, k - 1], recv_sem=g2r.at[d - 1, k - 1],
            device_id=(s, peer(k)), device_id_type=MESH,
        )

    for d in reach:
        @pl.when(s + d < n_seq)
        def _():
            along(d).start()

        @pl.when(s < d)
        def _():
            win[pl.ds((REACH - 1 - d) * tokens, tokens), :] = jnp.zeros((tokens, width), win.dtype)

    for d in reach:
        @pl.when(s >= d)
        def _():
            along(d).wait_recv()
            for k in peers:
                across(d, k).start()

    base = s * tokens - margin
    key = lax.broadcasted_iota(jnp.int32, (window, tokens), 0)
    last = margin + lax.broadcasted_iota(jnp.int32, (window, tokens), 1)
    bias[...] = jnp.where((key <= last) & (key >= first_ref[...] - base), 0.0, lowest)
    for copy in loads:
        copy.wait()

    @pl.loop(0, head_local)
    def _(i):
        load_q(i).wait()

    for d in reach:
        @pl.when(s >= d)
        def _():
            for k in peers:
                across(d, k).wait()

        @pl.when(s + d < n_seq)
        def _():
            along(d).wait_send()

    win_t[...] = win[...].T
    rate = softmax_scale * math.log2(math.e)

    def tile_products(i):
        rows = pl.ds(pl.multiple_of(i * tile_rows, tile_rows), tile_rows)
        scores = jnp.dot(win[...], q[:, rows], preferred_element_type=jnp.float32)
        grad_probs = lax.dot_general(
            win[:, :LAT], g[rows, :], contract_last, preferred_element_type=jnp.float32
        )
        return scores, grad_probs

    def tile_softmax(i, scores, grad_probs):
        for j in range(TILE_HEADS):
            part = slice(j * tokens, (j + 1) * tokens)
            lanes = pl.ds(pl.multiple_of(i * tile_rows + j * tokens, tokens), tokens)
            shown = scores[:, part] + bias[...]
            grads = grad_probs[:, part]
            top = jnp.max(shown, axis=0, keepdims=True)
            weights = jnp.exp2((shown - top) * rate)
            inverse = 1.0 / jnp.sum(weights, axis=0, keepdims=True)
            delta = jnp.sum(weights * grads, axis=0, keepdims=True) * inverse
            probs = weights * inverse
            ds[:, lanes] = (probs * (grads - delta)).astype(ds.dtype)
            pb[:, lanes] = probs.astype(pb.dtype)

    def softmax_pair(j, carry):
        first, second = tile_products(2 * j), tile_products(2 * j + 1)
        tile_softmax(2 * j, *first)
        tile_softmax(2 * j + 1, *second)
        return carry

    lax.fori_loop(0, n_tile // 2, softmax_pair, 0)

    def head_copy(c, k):
        return pltpu.make_async_remote_copy(
            src_ref=t_send[c].at[peer(k)], dst_ref=t_recv[c].at[k - 1],
            send_sem=r1s.at[c, k - 1], recv_sem=r1r.at[c, k - 1],
            device_id=(s, peer(k)), device_id_type=MESH,
        )

    def seq_copy(c, d):
        return pltpu.make_async_remote_copy(
            src_ref=r_send[c].at[d - 1], dst_ref=r_recv[c].at[d - 1],
            send_sem=r2s.at[c, d - 1], recv_sem=r2r.at[c, d - 1],
            device_id=(s - d, h), device_id_type=MESH,
        )

    def last_copy(c, k):
        return pltpu.make_async_remote_copy(
            src_ref=f_send[c], dst_ref=f_recv[c].at[k - 1],
            send_sem=r3s.at[c, k - 1], recv_sem=r3r.at[c, k - 1],
            device_id=(s, peer(k)), device_id_type=MESH,
        )

    def latent_part(c):
        low, high = cuts[c]
        split = min(high, LAT)
        term = lax.dot_general(
            ds[...], q[low:high, :], contract_last, preferred_element_type=jnp.float32
        ) * softmax_scale
        value = jnp.dot(pb[...], g[:, low:split], preferred_element_type=jnp.float32)
        if split < high:
            own[c][:, : split - low] = term[:, : split - low] + value
            own[c][:, split - low :] = term[:, split - low :]
        else:
            own[c][...] = term + value
        for j in range(n_head):
            for b in range(REACH):
                t_send[c][j, b * quarter : (b + 1) * quarter, :] = own[c][
                    b * tokens + j * quarter : b * tokens + (j + 1) * quarter, :
                ].astype(jnp.bfloat16)
        for k in peers:
            head_copy(c, k).start()

    def head_sum(c):
        for k in peers:
            head_copy(c, k).wait()
        for b in range(REACH):
            total = own[c][pl.ds(b * tokens + share, quarter), :]
            for k in peers:
                total = total + t_recv[c][k - 1, b * quarter : (b + 1) * quarter, :].astype(jnp.float32)
            d = REACH - 1 - b
            if d == 0:
                r_own[c][...] = total
            else:
                r_send[c][d - 1] = total.astype(jnp.bfloat16)

                @pl.when(s >= d)
                def _():
                    seq_copy(c, d).start()

    def seq_sum(c):
        for d in reach:
            @pl.when(s + d < n_seq)
            def _():
                seq_copy(c, d).wait_recv()
                r_own[c][...] = r_own[c][...] + r_recv[c][d - 1].astype(jnp.float32)

            @pl.when(s >= d)
            def _():
                seq_copy(c, d).wait_send()

        f_send[c][...] = r_own[c][...]
        for k in peers:
            last_copy(c, k).start()
        low, high = cuts[c]
        out_ref[pl.ds(share, quarter), low:high] = r_own[c][...]

    def collect(c):
        low, high = cuts[c]
        for k in peers:
            last_copy(c, k).wait()
            source = lax.rem(h + n_head - k, n_head)
            out_ref[pl.ds(pl.multiple_of(source * quarter, quarter), quarter), low:high] = f_recv[c][k - 1]

    def query_tile(i):
        rows = pl.ds(pl.multiple_of(i * tile_rows, tile_rows), tile_rows)
        part = jnp.dot(win_t[...], ds[:, rows], preferred_element_type=jnp.float32)
        part = (part * softmax_scale).astype(dq.dtype)
        for j in range(TILE_HEADS):
            dq[i * TILE_HEADS + j] = part[:, j * tokens : (j + 1) * tokens]

    def query_store(i):
        heads = pl.ds(i * TILE_HEADS, TILE_HEADS)
        return pltpu.make_async_copy(dq.at[heads], dq_hbm.at[heads], store_sem.at[i])

    def query_tiles(low, high):
        def one(i, carry):
            query_tile(i)
            query_store(i).start()
            return carry

        lax.fori_loop(low, high, one, 0)

    for c in range(n_cut):
        latent_part(c)
    query_tiles(0, n_tile // 4)
    head_sum(0)
    query_tiles(n_tile // 4, n_tile - n_tile // 4)
    for c in range(1, n_cut):
        head_sum(c)
    seq_sum(0)
    query_tiles(n_tile - n_tile // 4, n_tile)
    for c in range(1, n_cut):
        seq_sum(c)
    for c in range(n_cut):
        collect(c)
    for i in range(n_tile):
        query_store(i).wait()


def fused_per_device(n_seq, n_head, queries, latent_kv, grad_out, doc_start):
    tokens, head_local, width = queries.shape
    rows = tokens * head_local
    quarter = tokens // n_head
    cuts = ((LAT // 2, width), (0, LAT // 2))
    sizes = [high - low for low, high in cuts]
    bf, f32 = jnp.bfloat16, jnp.float32
    first = doc_start.reshape(1, tokens)
    window = REACH * tokens
    scratch = [
        pltpu.VMEM((width, rows), bf),
        pltpu.VMEM((rows, LAT), bf),
        pltpu.VMEM((head_local, width, tokens), bf),
        pltpu.VMEM((window, rows), bf),
        pltpu.VMEM((window, rows), bf),
        pltpu.VMEM((window, width), bf),
        pltpu.VMEM((width, window), bf),
        pltpu.VMEM((window, tokens), f32),
    ]
    scratch += [pltpu.VMEM((window, n), f32) for n in sizes]
    scratch += [pltpu.VMEM((n_head, REACH * quarter, n), bf) for n in sizes]
    scratch += [pltpu.VMEM((n_head - 1, REACH * quarter, n), bf) for n in sizes]
    scratch += [pltpu.VMEM((REACH - 1, quarter, n), bf) for n in sizes]
    scratch += [pltpu.VMEM((REACH - 1, quarter, n), bf) for n in sizes]
    scratch += [pltpu.VMEM((quarter, n), f32) for n in sizes]
    scratch += [pltpu.VMEM((quarter, n), f32) for n in sizes]
    scratch += [pltpu.VMEM((n_head - 1, quarter, n), f32) for n in sizes]
    dma = pltpu.SemaphoreType.DMA
    n_cut = len(cuts)
    scratch += [dma((2,)), dma((head_local,)), dma((head_local // TILE_HEADS,))]
    scratch += [dma((REACH - 1,)), dma((REACH - 1,))]
    scratch += [dma((REACH - 1, n_head - 1)), dma((REACH - 1, n_head - 1))]
    scratch += [dma((n_cut, n_head - 1)), dma((n_cut, n_head - 1))]
    scratch += [dma((n_cut, REACH - 1)), dma((n_cut, REACH - 1))]
    scratch += [dma((n_cut, n_head - 1)), dma((n_cut, n_head - 1))]

    def body(*refs):
        fused_kernel(n_seq, n_head, head_local, tokens, *refs[:14], cuts, *refs[14:])

    vmem = pl.BlockSpec(memory_space=pltpu.VMEM)
    anywhere = pl.BlockSpec(memory_space=pl.ANY)
    grad_rows, grad_latent = pl.pallas_call(
        body,
        out_shape=(
            jax.ShapeDtypeStruct((head_local, width, tokens), bf),
            jax.ShapeDtypeStruct((tokens, width), f32),
        ),
        in_specs=[anywhere, anywhere, vmem, vmem],
        out_specs=(anywhere, vmem),
        scratch_shapes=scratch,
        compiler_params=pltpu.CompilerParams(
            collective_id=0, has_side_effects=True, vmem_limit_bytes=60 * 1024 * 1024
        ),
    )(
        queries.transpose(1, 2, 0),
        grad_out.transpose(1, 0, 2).reshape(rows, LAT),
        latent_kv,
        first,
    )
    return grad_rows.transpose(2, 0, 1), grad_latent


def solution(mesh):
    in_specs = (P("seq", "head", None), P("seq", None), P("seq", "head", None), P("seq"))
    out_specs = (P("seq", "head", None), P("seq", None))
    n_seq, n_head = mesh.shape["seq"], mesh.shape["head"]

    def routed(queries, latent_kv, grad_out, doc_start):
        tokens, head_local, _ = queries.shape
        fits = (
            n_head > 1
            and tokens % 128 == 0
            and tokens % (16 * n_head) == 0
            and head_local % (2 * TILE_HEADS) == 0
            and n_seq >= REACH
        )
        run = partial(fused_per_device, n_seq, n_head) if fits else per_device
        return run(queries, latent_kv, grad_out, doc_start)

    return jax.shard_map(
        routed, mesh=mesh, in_specs=in_specs, out_specs=out_specs, check_vma=False
    )
```

```python
import math
from functools import partial

import jax
import jax.numpy as jnp
from jax import lax
from jax.experimental import pallas as pl
from jax.experimental.pallas import tpu as pltpu
from jax.sharding import PartitionSpec as P

LAT = 512
REACH = 4


softmax_scale = 192.0 ** (-0.5)
lowest = -1e30
contract_last = (((1,), (1,)), ((), ()))
contract_first = (((0,), (0,)), ((), ()))


def passed_along(block, axis, distance):
    devices = range(lax.axis_size(axis))
    route = [(i - distance, i) for i in devices if i - distance in devices]
    return lax.ppermute(block, axis, route)


def product_tiles(query_rows, grad_rows, kv_block, unused):
    scores = (
        lax.dot_general(query_rows, kv_block, contract_last, preferred_element_type=jnp.float32)
        * softmax_scale
    )
    grad_probs = lax.dot_general(
        grad_rows, kv_block[:, :LAT], contract_last, preferred_element_type=jnp.float32
    )
    return (scores, grad_probs)


def empty_tiles(query_count, key_count, unused):
    blank = jnp.zeros((query_count, key_count), jnp.float32)
    return (blank, blank)


def grads_update(
    query_rows, grad_rows, kv_block, scores, grad_probs, visible, log_total, row_delta, unused
):
    weights = jnp.where(visible, jnp.exp(scores - log_total[:, None]), 0.0)
    grad_bf = (weights * (grad_probs - row_delta[:, None])).astype(jnp.bfloat16)
    prob_bf = weights.astype(jnp.bfloat16)
    query_part = jnp.dot(grad_bf, kv_block, preferred_element_type=jnp.float32)
    from_scores = (
        lax.dot_general(grad_bf, query_rows, contract_first, preferred_element_type=jnp.float32)
        * softmax_scale
    )
    from_values = lax.dot_general(
        prob_bf, grad_rows, contract_first, preferred_element_type=jnp.float32
    )
    term = jnp.concatenate([from_scores[:, :LAT] + from_values, from_scores[:, LAT:]], axis=1)
    return (query_part, term)


def no_grads(query_count, tokens, row_width, unused):
    return (
        jnp.zeros((query_count, row_width), jnp.float32),
        jnp.zeros((tokens, row_width), jnp.float32),
    )


def per_device(queries, latent_kv, grad_out, doc_start):
    tokens, head_local, row_width = queries.shape
    query_count = tokens * head_local
    first_pos = lax.axis_index("seq") * tokens
    query_rows = queries.reshape(query_count, row_width)
    grad_rows = grad_out.reshape(query_count, LAT)
    row_pos = jnp.repeat(first_pos + jnp.arange(tokens, dtype=jnp.int32), head_local)
    row_first = jnp.repeat(doc_start, head_local)
    low_first = jnp.min(doc_start)
    windows = [latent_kv]
    for distance in range(1, REACH):
        windows.append(passed_along(latent_kv, "seq", distance))
    key_starts = [first_pos - distance * tokens for distance in range(REACH)]
    wanted = [start + tokens > low_first for start in key_starts]
    blank = jnp.zeros((query_count,), jnp.float32)
    row_top = jnp.full((query_count,), lowest, jnp.float32)
    total_exp = blank
    weighted = blank
    kept = []
    for distance in range(REACH):
        scores, grad_probs = lax.cond(
            wanted[distance],
            partial(product_tiles, query_rows, grad_rows, windows[distance]),
            partial(empty_tiles, query_count, tokens),
            0,
        )
        key_pos = key_starts[distance] + jnp.arange(tokens, dtype=jnp.int32)
        visible = (key_pos[None, :] <= row_pos[:, None]) & (key_pos[None, :] >= row_first[:, None])
        new_top = jnp.maximum(row_top, jnp.max(jnp.where(visible, scores, lowest), axis=1))
        rescale = jnp.exp(row_top - new_top)
        weights = jnp.where(visible, jnp.exp(scores - new_top[:, None]), 0.0)
        total_exp = total_exp * rescale + jnp.sum(weights, axis=1)
        weighted = weighted * rescale + jnp.sum(weights * grad_probs, axis=1)
        row_top = new_top
        kept.append((scores, grad_probs, visible))
    log_total = row_top + jnp.log(total_exp)
    row_delta = weighted / total_exp
    query_grad = jnp.zeros((query_count, row_width), jnp.float32)
    terms = []
    for distance in range(REACH):
        scores, grad_probs, visible = kept[distance]
        compute = partial(
            grads_update,
            query_rows,
            grad_rows,
            windows[distance],
            scores,
            grad_probs,
            visible,
            log_total,
            row_delta,
        )
        query_part, term = lax.cond(
            wanted[distance], compute, partial(no_grads, query_count, tokens, row_width), 0
        )
        query_grad = query_grad + query_part
        terms.append(term)
    own_rows = terms[0]
    for distance in range(1, REACH):
        own_rows = own_rows + passed_along(
            terms[distance].astype(jnp.bfloat16), "seq", -distance
        ).astype(jnp.float32)
    grad_latent = lax.psum(own_rows, "head")
    grad_queries = (
        (softmax_scale * query_grad).astype(jnp.bfloat16).reshape(tokens, head_local, row_width)
    )
    return (grad_queries, grad_latent)


TILE_HEADS = 4
MESH = pl.DeviceIdType.MESH


def fused_kernel(
    n_seq, n_head, head_local, tokens,
    q_hbm, g_hbm, kv_t_ref, first_ref,
    dq_hbm, out_ref,
    q, g_in, g, out_rows, dq, ds, pb, win, win_t, bias, parts, *rest,
):
    cuts = parts
    n_cut = len(cuts)
    take = iter(rest)
    own = [next(take) for _ in range(n_cut)]
    t_send = [next(take) for _ in range(n_cut)]
    t_recv = [next(take) for _ in range(n_cut)]
    r_send = [next(take) for _ in range(n_cut)]
    r_recv = [next(take) for _ in range(n_cut)]
    r_own = [next(take) for _ in range(n_cut)]
    f_send = [next(take) for _ in range(n_cut)]
    f_recv = [next(take) for _ in range(n_cut)]
    (load_sem, q_sem, store_sem, g1s, g1r, g2s, g2r, r1s, r1r, r2s, r2r, r3s, r3r) = take

    s = lax.axis_index("seq")
    h = lax.axis_index("head")
    width = kv_t_ref.shape[0]
    quarter = tokens // n_head
    tile_rows = TILE_HEADS * tokens
    n_tile = head_local // TILE_HEADS
    margin = (REACH - 1) * tokens
    window = REACH * tokens
    peers = range(1, n_head)
    reach = range(1, REACH)

    def peer(k):
        return lax.rem(h + k, n_head)

    def load_q(i):
        lanes = pl.ds(pl.multiple_of(i * tokens, tokens), tokens)
        return pltpu.make_async_copy(q_hbm.at[i], q.at[:, lanes], q_sem.at[i])

    def load_g(i):
        toks = pl.ds(i * half, half)
        return pltpu.make_async_copy(g_hbm.at[toks], g_in.at[toks], load_sem.at[i])

    half = tokens // 2
    for i in range(2):
        load_g(i).start()

    @pl.loop(0, head_local)
    def _(i):
        load_q(i).start()

    win[margin:, :] = kv_t_ref[...].T
    barrier = pltpu.get_barrier_semaphore()
    for k in peers:
        pl.semaphore_signal(barrier, inc=1, device_id=(s, peer(k)), device_id_type=MESH)
    for d in reach:
        @pl.when(s >= d)
        def _():
            pl.semaphore_signal(barrier, inc=1, device_id=(s - d, h), device_id_type=MESH)

        @pl.when(s + d < n_seq)
        def _():
            pl.semaphore_signal(barrier, inc=1, device_id=(s + d, h), device_id_type=MESH)

    before = jnp.minimum(s, REACH - 1)
    after = jnp.minimum(n_seq - 1 - s, REACH - 1)
    pl.semaphore_wait(barrier, n_head - 1 + before + after)

    share = pl.multiple_of(h * quarter, quarter)

    def along(d):
        return pltpu.make_async_remote_copy(
            src_ref=win.at[pl.ds(margin + share, quarter)],
            dst_ref=win.at[pl.ds((REACH - 1 - d) * tokens + share, quarter)],
            send_sem=g1s.at[d - 1], recv_sem=g1r.at[d - 1],
            device_id=(s + d, h), device_id_type=MESH,
        )

    def across(d, k):
        rows = pl.ds((REACH - 1 - d) * tokens + share, quarter)
        return pltpu.make_async_remote_copy(
            src_ref=win.at[rows], dst_ref=win.at[rows],
            send_sem=g2s.at[d - 1, k - 1], recv_sem=g2r.at[d - 1, k - 1],
            device_id=(s, peer(k)), device_id_type=MESH,
        )

    for d in reach:
        @pl.when(s + d < n_seq)
        def _():
            along(d).start()

        @pl.when(s < d)
        def _():
            win[pl.ds((REACH - 1 - d) * tokens, tokens), :] = jnp.zeros((tokens, width), win.dtype)

    base = s * tokens - margin
    key = lax.broadcasted_iota(jnp.int32, (window, tokens), 0)
    last = margin + lax.broadcasted_iota(jnp.int32, (window, tokens), 1)
    bias[...] = jnp.where((key <= last) & (key >= first_ref[...] - base), 0.0, lowest)
    def by_head(i):
        load_g(i).wait()

        @pl.loop(0, half // 16)
        def _(j):
            toks = pl.ds(pl.multiple_of(i * half + j * 16, 16), 16)
            block = g_in[toks].astype(jnp.float32)
            g[:, toks, :] = jnp.swapaxes(block, 0, 1).astype(g.dtype)

    by_head(0)
    for d in reach:
        @pl.when(s >= d)
        def _():
            along(d).wait_recv()
            for k in peers:
                across(d, k).start()

    by_head(1)

    @pl.loop(0, head_local)
    def _(i):
        load_q(i).wait()

    for d in reach:
        @pl.when(s >= d)
        def _():
            for k in peers:
                across(d, k).wait()

        @pl.when(s + d < n_seq)
        def _():
            along(d).wait_send()

    win_t[...] = win[...].T
    rate = softmax_scale * math.log2(math.e)

    def tile_products(i):
        rows = pl.ds(pl.multiple_of(i * tile_rows, tile_rows), tile_rows)
        scores = jnp.dot(win[...], q[:, rows], preferred_element_type=jnp.float32)
        grad_probs = lax.dot_general(
            win[:, :LAT], g[pl.ds(i * TILE_HEADS, TILE_HEADS)].reshape(tile_rows, LAT), contract_last, preferred_element_type=jnp.float32
        )
        return scores, grad_probs

    def tile_softmax(i, scores, grad_probs):
        for j in range(TILE_HEADS):
            part = slice(j * tokens, (j + 1) * tokens)
            lanes = pl.ds(pl.multiple_of(i * tile_rows + j * tokens, tokens), tokens)
            shown = scores[:, part] + bias[...]
            grads = grad_probs[:, part]
            top = jnp.max(shown, axis=0, keepdims=True)
            weights = jnp.exp2((shown - top) * rate)
            inverse = 1.0 / jnp.sum(weights, axis=0, keepdims=True)
            delta = jnp.sum(weights * grads, axis=0, keepdims=True) * inverse
            probs = weights * inverse
            ds[:, lanes] = (probs * (grads - delta)).astype(ds.dtype)
            pb[:, lanes] = probs.astype(pb.dtype)

    def softmax_pair(j, carry):
        first, second = tile_products(2 * j), tile_products(2 * j + 1)
        tile_softmax(2 * j, *first)
        tile_softmax(2 * j + 1, *second)
        return carry

    lax.fori_loop(0, n_tile // 2, softmax_pair, 0)

    def head_copy(c, k):
        return pltpu.make_async_remote_copy(
            src_ref=t_send[c].at[peer(k)], dst_ref=t_recv[c].at[k - 1],
            send_sem=r1s.at[c, k - 1], recv_sem=r1r.at[c, k - 1],
            device_id=(s, peer(k)), device_id_type=MESH,
        )

    def seq_copy(c, d):
        return pltpu.make_async_remote_copy(
            src_ref=r_send[c].at[d - 1], dst_ref=r_recv[c].at[d - 1],
            send_sem=r2s.at[c, d - 1], recv_sem=r2r.at[c, d - 1],
            device_id=(s - d, h), device_id_type=MESH,
        )

    def last_copy(c, k):
        return pltpu.make_async_remote_copy(
            src_ref=f_send[c], dst_ref=f_recv[c].at[k - 1],
            send_sem=r3s.at[c, k - 1], recv_sem=r3r.at[c, k - 1],
            device_id=(s, peer(k)), device_id_type=MESH,
        )

    def latent_part(c):
        low, high = cuts[c]
        split = min(high, LAT)
        term = lax.dot_general(
            ds[...], q[low:high, :], contract_last, preferred_element_type=jnp.float32
        ) * softmax_scale
        grads = g[:, :, low:split].reshape(head_local * tokens, split - low)
        value = jnp.dot(pb[...], grads, preferred_element_type=jnp.float32)
        if split < high:
            own[c][:, : split - low] = term[:, : split - low] + value
            own[c][:, split - low :] = term[:, split - low :]
        else:
            own[c][...] = term + value
        for j in range(n_head):
            for b in range(REACH):
                t_send[c][j, b * quarter : (b + 1) * quarter, :] = own[c][
                    b * tokens + j * quarter : b * tokens + (j + 1) * quarter, :
                ].astype(jnp.bfloat16)
        for k in peers:
            head_copy(c, k).start()

    def head_sum(c):
        for k in peers:
            head_copy(c, k).wait()
        for b in range(REACH):
            total = own[c][pl.ds(b * tokens + share, quarter), :]
            for k in peers:
                total = total + t_recv[c][k - 1, b * quarter : (b + 1) * quarter, :].astype(jnp.float32)
            d = REACH - 1 - b
            if d == 0:
                r_own[c][...] = total
            else:
                r_send[c][d - 1] = total.astype(jnp.bfloat16)

                @pl.when(s >= d)
                def _():
                    seq_copy(c, d).start()

    def seq_sum(c):
        for d in reach:
            @pl.when(s + d < n_seq)
            def _():
                seq_copy(c, d).wait_recv()
                r_own[c][...] = r_own[c][...] + r_recv[c][d - 1].astype(jnp.float32)

            @pl.when(s >= d)
            def _():
                seq_copy(c, d).wait_send()

        f_send[c][...] = r_own[c][...]
        for k in peers:
            last_copy(c, k).start()
        low, high = cuts[c]
        out_rows[pl.ds(share, quarter), low:high] = r_own[c][...]

    def collect(c):
        low, high = cuts[c]
        for k in peers:
            last_copy(c, k).wait()
            source = lax.rem(h + n_head - k, n_head)
            out_rows[pl.ds(pl.multiple_of(source * quarter, quarter), quarter), low:high] = f_recv[c][k - 1]

    def query_tile(i):
        rows = pl.ds(pl.multiple_of(i * tile_rows, tile_rows), tile_rows)
        part = jnp.dot(win_t[...], ds[:, rows], preferred_element_type=jnp.float32)
        part = (part * softmax_scale).astype(dq.dtype)
        for j in range(TILE_HEADS):
            dq[i * TILE_HEADS + j] = part[:, j * tokens : (j + 1) * tokens]

    def query_store(i):
        heads = pl.ds(i * TILE_HEADS, TILE_HEADS)
        return pltpu.make_async_copy(dq.at[heads], dq_hbm.at[heads], store_sem.at[i])

    def query_tiles(low, high):
        def one(i, carry):
            query_tile(i)
            query_store(i).start()
            return carry

        lax.fori_loop(low, high, one, 0)

    for c in range(n_cut):
        latent_part(c)
    query_tiles(0, n_tile // 4)
    head_sum(0)
    query_tiles(n_tile // 4, n_tile - n_tile // 4)
    for c in range(1, n_cut):
        head_sum(c)
    seq_sum(0)
    query_tiles(n_tile - n_tile // 4, n_tile)
    for c in range(1, n_cut):
        seq_sum(c)
    for c in range(n_cut):
        collect(c)
    out_ref[...] = out_rows[...].T
    for i in range(n_tile):
        query_store(i).wait()


def fused_per_device(n_seq, n_head, queries, latent_kv, grad_out, doc_start):
    tokens, head_local, width = queries.shape
    rows = tokens * head_local
    quarter = tokens // n_head
    cuts = ((LAT // 2, width), (0, LAT // 2))
    sizes = [high - low for low, high in cuts]
    bf, f32 = jnp.bfloat16, jnp.float32
    first = doc_start.reshape(1, tokens)
    window = REACH * tokens
    scratch = [
        pltpu.VMEM((width, rows), bf),
        pltpu.VMEM((tokens, head_local, LAT), bf),
        pltpu.VMEM((head_local, tokens, LAT), bf),
        pltpu.VMEM((tokens, width), f32),
        pltpu.VMEM((head_local, width, tokens), bf),
        pltpu.VMEM((window, rows), bf),
        pltpu.VMEM((window, rows), bf),
        pltpu.VMEM((window, width), bf),
        pltpu.VMEM((width, window), bf),
        pltpu.VMEM((window, tokens), f32),
    ]
    scratch += [pltpu.VMEM((window, n), f32) for n in sizes]
    scratch += [pltpu.VMEM((n_head, REACH * quarter, n), bf) for n in sizes]
    scratch += [pltpu.VMEM((n_head - 1, REACH * quarter, n), bf) for n in sizes]
    scratch += [pltpu.VMEM((REACH - 1, quarter, n), bf) for n in sizes]
    scratch += [pltpu.VMEM((REACH - 1, quarter, n), bf) for n in sizes]
    scratch += [pltpu.VMEM((quarter, n), f32) for n in sizes]
    scratch += [pltpu.VMEM((quarter, n), f32) for n in sizes]
    scratch += [pltpu.VMEM((n_head - 1, quarter, n), f32) for n in sizes]
    dma = pltpu.SemaphoreType.DMA
    n_cut = len(cuts)
    scratch += [dma((2,)), dma((head_local,)), dma((head_local // TILE_HEADS,))]
    scratch += [dma((REACH - 1,)), dma((REACH - 1,))]
    scratch += [dma((REACH - 1, n_head - 1)), dma((REACH - 1, n_head - 1))]
    scratch += [dma((n_cut, n_head - 1)), dma((n_cut, n_head - 1))]
    scratch += [dma((n_cut, REACH - 1)), dma((n_cut, REACH - 1))]
    scratch += [dma((n_cut, n_head - 1)), dma((n_cut, n_head - 1))]

    def body(*refs):
        fused_kernel(n_seq, n_head, head_local, tokens, *refs[:16], cuts, *refs[16:])

    vmem = pl.BlockSpec(memory_space=pltpu.VMEM)
    anywhere = pl.BlockSpec(memory_space=pl.ANY)
    grad_rows, grad_latent = pl.pallas_call(
        body,
        out_shape=(
            jax.ShapeDtypeStruct((head_local, width, tokens), bf),
            jax.ShapeDtypeStruct((width, tokens), f32),
        ),
        in_specs=[anywhere, anywhere, vmem, vmem],
        out_specs=(anywhere, vmem),
        scratch_shapes=scratch,
        compiler_params=pltpu.CompilerParams(
            collective_id=0, has_side_effects=True, vmem_limit_bytes=60 * 1024 * 1024
        ),
    )(
        queries.transpose(1, 2, 0),
        grad_out,
        latent_kv.T,
        first,
    )
    return grad_rows.transpose(2, 0, 1), grad_latent.T


def solution(mesh):
    in_specs = (P("seq", "head", None), P("seq", None), P("seq", "head", None), P("seq"))
    out_specs = (P("seq", "head", None), P("seq", None))
    n_seq, n_head = mesh.shape["seq"], mesh.shape["head"]

    def routed(queries, latent_kv, grad_out, doc_start):
        tokens, head_local, _ = queries.shape
        fits = (
            n_head > 1
            and tokens % 128 == 0
            and tokens % (16 * n_head) == 0
            and head_local % (2 * TILE_HEADS) == 0
            and n_seq >= REACH
        )
        run = partial(fused_per_device, n_seq, n_head) if fits else per_device
        return run(queries, latent_kv, grad_out, doc_start)

    return jax.shard_map(
        routed, mesh=mesh, in_specs=in_specs, out_specs=out_specs, check_vma=False
    )
```

```python
import math
from functools import partial

import jax
import jax.numpy as jnp
from jax import lax
from jax.experimental import pallas as pl
from jax.experimental.pallas import tpu as pltpu
from jax.sharding import PartitionSpec as P

LAT = 512
REACH = 4


softmax_scale = 192.0 ** (-0.5)
lowest = -1e30
contract_last = (((1,), (1,)), ((), ()))
contract_first = (((0,), (0,)), ((), ()))


def passed_along(block, axis, distance):
    devices = range(lax.axis_size(axis))
    route = [(i - distance, i) for i in devices if i - distance in devices]
    return lax.ppermute(block, axis, route)


def product_tiles(query_rows, grad_rows, kv_block, unused):
    scores = (
        lax.dot_general(query_rows, kv_block, contract_last, preferred_element_type=jnp.float32)
        * softmax_scale
    )
    grad_probs = lax.dot_general(
        grad_rows, kv_block[:, :LAT], contract_last, preferred_element_type=jnp.float32
    )
    return (scores, grad_probs)


def empty_tiles(query_count, key_count, unused):
    blank = jnp.zeros((query_count, key_count), jnp.float32)
    return (blank, blank)


def grads_update(
    query_rows, grad_rows, kv_block, scores, grad_probs, visible, log_total, row_delta, unused
):
    weights = jnp.where(visible, jnp.exp(scores - log_total[:, None]), 0.0)
    grad_bf = (weights * (grad_probs - row_delta[:, None])).astype(jnp.bfloat16)
    prob_bf = weights.astype(jnp.bfloat16)
    query_part = jnp.dot(grad_bf, kv_block, preferred_element_type=jnp.float32)
    from_scores = (
        lax.dot_general(grad_bf, query_rows, contract_first, preferred_element_type=jnp.float32)
        * softmax_scale
    )
    from_values = lax.dot_general(
        prob_bf, grad_rows, contract_first, preferred_element_type=jnp.float32
    )
    term = jnp.concatenate([from_scores[:, :LAT] + from_values, from_scores[:, LAT:]], axis=1)
    return (query_part, term)


def no_grads(query_count, tokens, row_width, unused):
    return (
        jnp.zeros((query_count, row_width), jnp.float32),
        jnp.zeros((tokens, row_width), jnp.float32),
    )


def per_device(queries, latent_kv, grad_out, doc_start):
    tokens, head_local, row_width = queries.shape
    query_count = tokens * head_local
    first_pos = lax.axis_index("seq") * tokens
    query_rows = queries.reshape(query_count, row_width)
    grad_rows = grad_out.reshape(query_count, LAT)
    row_pos = jnp.repeat(first_pos + jnp.arange(tokens, dtype=jnp.int32), head_local)
    row_first = jnp.repeat(doc_start, head_local)
    low_first = jnp.min(doc_start)
    windows = [latent_kv]
    for distance in range(1, REACH):
        windows.append(passed_along(latent_kv, "seq", distance))
    key_starts = [first_pos - distance * tokens for distance in range(REACH)]
    wanted = [start + tokens > low_first for start in key_starts]
    blank = jnp.zeros((query_count,), jnp.float32)
    row_top = jnp.full((query_count,), lowest, jnp.float32)
    total_exp = blank
    weighted = blank
    kept = []
    for distance in range(REACH):
        scores, grad_probs = lax.cond(
            wanted[distance],
            partial(product_tiles, query_rows, grad_rows, windows[distance]),
            partial(empty_tiles, query_count, tokens),
            0,
        )
        key_pos = key_starts[distance] + jnp.arange(tokens, dtype=jnp.int32)
        visible = (key_pos[None, :] <= row_pos[:, None]) & (key_pos[None, :] >= row_first[:, None])
        new_top = jnp.maximum(row_top, jnp.max(jnp.where(visible, scores, lowest), axis=1))
        rescale = jnp.exp(row_top - new_top)
        weights = jnp.where(visible, jnp.exp(scores - new_top[:, None]), 0.0)
        total_exp = total_exp * rescale + jnp.sum(weights, axis=1)
        weighted = weighted * rescale + jnp.sum(weights * grad_probs, axis=1)
        row_top = new_top
        kept.append((scores, grad_probs, visible))
    log_total = row_top + jnp.log(total_exp)
    row_delta = weighted / total_exp
    query_grad = jnp.zeros((query_count, row_width), jnp.float32)
    terms = []
    for distance in range(REACH):
        scores, grad_probs, visible = kept[distance]
        compute = partial(
            grads_update,
            query_rows,
            grad_rows,
            windows[distance],
            scores,
            grad_probs,
            visible,
            log_total,
            row_delta,
        )
        query_part, term = lax.cond(
            wanted[distance], compute, partial(no_grads, query_count, tokens, row_width), 0
        )
        query_grad = query_grad + query_part
        terms.append(term)
    own_rows = terms[0]
    for distance in range(1, REACH):
        own_rows = own_rows + passed_along(
            terms[distance].astype(jnp.bfloat16), "seq", -distance
        ).astype(jnp.float32)
    grad_latent = lax.psum(own_rows, "head")
    grad_queries = (
        (softmax_scale * query_grad).astype(jnp.bfloat16).reshape(tokens, head_local, row_width)
    )
    return (grad_queries, grad_latent)


TILE_HEADS = 4
MESH = pl.DeviceIdType.MESH


def fused_kernel(
    n_seq, n_head, head_local, tokens,
    q_hbm, g_hbm, kv_t_ref, first_ref,
    dq_hbm, out_ref,
    q, g_in, g, out_rows, dq, ds, pb, win, win_t, bias, parts, *rest,
):
    cuts = parts
    n_cut = len(cuts)
    take = iter(rest)
    own = [next(take) for _ in range(n_cut)]
    t_send = [next(take) for _ in range(n_cut)]
    t_recv = [next(take) for _ in range(n_cut)]
    r_send = [next(take) for _ in range(n_cut)]
    r_recv = [next(take) for _ in range(n_cut)]
    r_own = [next(take) for _ in range(n_cut)]
    f_send = [next(take) for _ in range(n_cut)]
    f_recv = [next(take) for _ in range(n_cut)]
    (load_sem, q_sem, store_sem, g1s, g1r, g2s, g2r, r1s, r1r, r2s, r2r, r3s, r3r) = take

    s = lax.axis_index("seq")
    h = lax.axis_index("head")
    width = kv_t_ref.shape[0]
    quarter = tokens // n_head
    tile_rows = TILE_HEADS * tokens
    n_tile = head_local // TILE_HEADS
    margin = (REACH - 1) * tokens
    window = REACH * tokens
    peers = range(1, n_head)
    reach = range(1, REACH)

    def peer(k):
        return lax.rem(h + k, n_head)

    def load_q(i):
        lanes = pl.ds(pl.multiple_of(i * tokens, tokens), tokens)
        return pltpu.make_async_copy(q_hbm.at[i], q.at[:, lanes], q_sem.at[i])

    def load_g(i):
        toks = pl.ds(i * half, half)
        return pltpu.make_async_copy(g_hbm.at[toks], g_in.at[toks], load_sem.at[i])

    half = tokens // 2
    for i in range(2):
        load_g(i).start()

    @pl.loop(0, head_local)
    def _(i):
        load_q(i).start()

    win[margin:, :] = kv_t_ref[...].T
    barrier = pltpu.get_barrier_semaphore()
    for k in peers:
        pl.semaphore_signal(barrier, inc=1, device_id=(s, peer(k)), device_id_type=MESH)
    for d in reach:
        @pl.when(s >= d)
        def _():
            pl.semaphore_signal(barrier, inc=1, device_id=(s - d, h), device_id_type=MESH)

        @pl.when(s + d < n_seq)
        def _():
            pl.semaphore_signal(barrier, inc=1, device_id=(s + d, h), device_id_type=MESH)

    before = jnp.minimum(s, REACH - 1)
    after = jnp.minimum(n_seq - 1 - s, REACH - 1)
    pl.semaphore_wait(barrier, n_head - 1 + before + after)

    share = pl.multiple_of(h * quarter, quarter)

    def along(d):
        return pltpu.make_async_remote_copy(
            src_ref=win.at[pl.ds(margin + share, quarter)],
            dst_ref=win.at[pl.ds((REACH - 1 - d) * tokens + share, quarter)],
            send_sem=g1s.at[d - 1], recv_sem=g1r.at[d - 1],
            device_id=(s + d, h), device_id_type=MESH,
        )

    def across(d, k):
        rows = pl.ds((REACH - 1 - d) * tokens + share, quarter)
        return pltpu.make_async_remote_copy(
            src_ref=win.at[rows], dst_ref=win.at[rows],
            send_sem=g2s.at[d - 1, k - 1], recv_sem=g2r.at[d - 1, k - 1],
            device_id=(s, peer(k)), device_id_type=MESH,
        )

    for d in reach:
        @pl.when(s + d < n_seq)
        def _():
            along(d).start()

        @pl.when(s < d)
        def _():
            win[pl.ds((REACH - 1 - d) * tokens, tokens), :] = jnp.zeros((tokens, width), win.dtype)

    base = s * tokens - margin
    key = lax.broadcasted_iota(jnp.int32, (window, tokens), 0)
    last = margin + lax.broadcasted_iota(jnp.int32, (window, tokens), 1)
    bias[...] = jnp.where((key <= last) & (key >= first_ref[...] - base), 0.0, lowest)
    def by_head(i):
        load_g(i).wait()

        @pl.loop(0, half // 16)
        def _(j):
            toks = pl.ds(pl.multiple_of(i * half + j * 16, 16), 16)
            block = g_in[toks].astype(jnp.float32)
            g[:, toks, :] = jnp.swapaxes(block, 0, 1).astype(g.dtype)

    by_head(0)
    for d in reach:
        @pl.when(s >= d)
        def _():
            along(d).wait_recv()
            for k in peers:
                across(d, k).start()

    by_head(1)

    @pl.loop(0, head_local)
    def _(i):
        load_q(i).wait()

    for d in reach:
        @pl.when(s >= d)
        def _():
            for k in peers:
                across(d, k).wait()

        @pl.when(s + d < n_seq)
        def _():
            along(d).wait_send()

    win_t[...] = win[...].T
    rate = softmax_scale * math.log2(math.e)

    def tile_products(i):
        rows = pl.ds(pl.multiple_of(i * tile_rows, tile_rows), tile_rows)
        scores = jnp.dot(win[...], q[:, rows], preferred_element_type=jnp.float32)
        grad_probs = lax.dot_general(
            win[:, :LAT], g[pl.ds(i * TILE_HEADS, TILE_HEADS)].reshape(tile_rows, LAT), contract_last, preferred_element_type=jnp.float32
        )
        return scores, grad_probs

    def tile_softmax(i, scores, grad_probs):
        for j in range(TILE_HEADS):
            part = slice(j * tokens, (j + 1) * tokens)
            lanes = pl.ds(pl.multiple_of(i * tile_rows + j * tokens, tokens), tokens)
            shown = scores[:, part] + bias[...]
            grads = grad_probs[:, part]
            top = jnp.max(shown, axis=0, keepdims=True)
            weights = jnp.exp2((shown - top) * rate)
            inverse = 1.0 / jnp.sum(weights, axis=0, keepdims=True)
            delta = jnp.sum(weights * grads, axis=0, keepdims=True) * inverse
            probs = weights * inverse
            ds[:, lanes] = (probs * (grads - delta)).astype(ds.dtype)
            pb[:, lanes] = probs.astype(pb.dtype)

    def softmax_pair(j, carry):
        first, second = tile_products(2 * j), tile_products(2 * j + 1)
        tile_softmax(2 * j, *first)
        tile_softmax(2 * j + 1, *second)
        return carry

    lax.fori_loop(0, n_tile // 2, softmax_pair, 0, unroll=2)

    def head_copy(c, k):
        return pltpu.make_async_remote_copy(
            src_ref=t_send[c].at[peer(k)], dst_ref=t_recv[c].at[k - 1],
            send_sem=r1s.at[c, k - 1], recv_sem=r1r.at[c, k - 1],
            device_id=(s, peer(k)), device_id_type=MESH,
        )

    def seq_copy(c, d):
        return pltpu.make_async_remote_copy(
            src_ref=r_send[c].at[d - 1], dst_ref=r_recv[c].at[d - 1],
            send_sem=r2s.at[c, d - 1], recv_sem=r2r.at[c, d - 1],
            device_id=(s - d, h), device_id_type=MESH,
        )

    def last_copy(c, k):
        return pltpu.make_async_remote_copy(
            src_ref=f_send[c], dst_ref=f_recv[c].at[k - 1],
            send_sem=r3s.at[c, k - 1], recv_sem=r3r.at[c, k - 1],
            device_id=(s, peer(k)), device_id_type=MESH,
        )

    def latent_part(c):
        low, high = cuts[c]
        split = min(high, LAT)
        term = lax.dot_general(
            ds[...], q[low:high, :], contract_last, preferred_element_type=jnp.float32
        ) * softmax_scale
        grads = g[:, :, low:split].reshape(head_local * tokens, split - low)
        value = jnp.dot(pb[...], grads, preferred_element_type=jnp.float32)
        if split < high:
            own[c][:, : split - low] = term[:, : split - low] + value
            own[c][:, split - low :] = term[:, split - low :]
        else:
            own[c][...] = term + value
        for j in range(n_head):
            for b in range(REACH):
                t_send[c][j, b * quarter : (b + 1) * quarter, :] = own[c][
                    b * tokens + j * quarter : b * tokens + (j + 1) * quarter, :
                ].astype(jnp.bfloat16)
        for k in peers:
            head_copy(c, k).start()

    def head_sum(c):
        for k in peers:
            head_copy(c, k).wait()
        for b in range(REACH):
            total = own[c][pl.ds(b * tokens + share, quarter), :]
            for k in peers:
                total = total + t_recv[c][k - 1, b * quarter : (b + 1) * quarter, :].astype(jnp.float32)
            d = REACH - 1 - b
            if d == 0:
                r_own[c][...] = total
            else:
                r_send[c][d - 1] = total.astype(jnp.bfloat16)

                @pl.when(s >= d)
                def _():
                    seq_copy(c, d).start()

    def seq_sum(c):
        for d in reach:
            @pl.when(s + d < n_seq)
            def _():
                seq_copy(c, d).wait_recv()
                r_own[c][...] = r_own[c][...] + r_recv[c][d - 1].astype(jnp.float32)

            @pl.when(s >= d)
            def _():
                seq_copy(c, d).wait_send()

        f_send[c][...] = r_own[c][...]
        for k in peers:
            last_copy(c, k).start()
        low, high = cuts[c]
        out_rows[pl.ds(share, quarter), low:high] = r_own[c][...]

    def collect(c):
        low, high = cuts[c]
        for k in peers:
            last_copy(c, k).wait()
            source = lax.rem(h + n_head - k, n_head)
            out_rows[pl.ds(pl.multiple_of(source * quarter, quarter), quarter), low:high] = f_recv[c][k - 1]

    def query_tile(i):
        rows = pl.ds(pl.multiple_of(i * tile_rows, tile_rows), tile_rows)
        part = jnp.dot(win_t[...], ds[:, rows], preferred_element_type=jnp.float32)
        part = (part * softmax_scale).astype(dq.dtype)
        for j in range(TILE_HEADS):
            dq[i * TILE_HEADS + j] = part[:, j * tokens : (j + 1) * tokens]

    def query_store(i):
        heads = pl.ds(i * TILE_HEADS, TILE_HEADS)
        return pltpu.make_async_copy(dq.at[heads], dq_hbm.at[heads], store_sem.at[i])

    def query_tiles(low, high):
        def one(i, carry):
            query_tile(i)
            query_store(i).start()
            return carry

        lax.fori_loop(low, high, one, 0, unroll=2)

    for c in range(n_cut):
        latent_part(c)
    query_tiles(0, n_tile // 4)
    head_sum(0)
    query_tiles(n_tile // 4, n_tile - n_tile // 4)
    for c in range(1, n_cut):
        head_sum(c)
    seq_sum(0)
    query_tiles(n_tile - n_tile // 4, n_tile)
    for c in range(1, n_cut):
        seq_sum(c)
    for c in range(n_cut):
        collect(c)
    out_ref[...] = out_rows[...].T
    for i in range(n_tile):
        query_store(i).wait()


def fused_per_device(n_seq, n_head, queries, latent_kv, grad_out, doc_start):
    tokens, head_local, width = queries.shape
    rows = tokens * head_local
    quarter = tokens // n_head
    cuts = ((LAT // 2, width), (0, LAT // 2))
    sizes = [high - low for low, high in cuts]
    bf, f32 = jnp.bfloat16, jnp.float32
    first = doc_start.reshape(1, tokens)
    window = REACH * tokens
    scratch = [
        pltpu.VMEM((width, rows), bf),
        pltpu.VMEM((tokens, head_local, LAT), bf),
        pltpu.VMEM((head_local, tokens, LAT), bf),
        pltpu.VMEM((tokens, width), f32),
        pltpu.VMEM((head_local, width, tokens), bf),
        pltpu.VMEM((window, rows), bf),
        pltpu.VMEM((window, rows), bf),
        pltpu.VMEM((window, width), bf),
        pltpu.VMEM((width, window), bf),
        pltpu.VMEM((window, tokens), f32),
    ]
    scratch += [pltpu.VMEM((window, n), f32) for n in sizes]
    scratch += [pltpu.VMEM((n_head, REACH * quarter, n), bf) for n in sizes]
    scratch += [pltpu.VMEM((n_head - 1, REACH * quarter, n), bf) for n in sizes]
    scratch += [pltpu.VMEM((REACH - 1, quarter, n), bf) for n in sizes]
    scratch += [pltpu.VMEM((REACH - 1, quarter, n), bf) for n in sizes]
    scratch += [pltpu.VMEM((quarter, n), f32) for n in sizes]
    scratch += [pltpu.VMEM((quarter, n), f32) for n in sizes]
    scratch += [pltpu.VMEM((n_head - 1, quarter, n), f32) for n in sizes]
    dma = pltpu.SemaphoreType.DMA
    n_cut = len(cuts)
    scratch += [dma((2,)), dma((head_local,)), dma((head_local // TILE_HEADS,))]
    scratch += [dma((REACH - 1,)), dma((REACH - 1,))]
    scratch += [dma((REACH - 1, n_head - 1)), dma((REACH - 1, n_head - 1))]
    scratch += [dma((n_cut, n_head - 1)), dma((n_cut, n_head - 1))]
    scratch += [dma((n_cut, REACH - 1)), dma((n_cut, REACH - 1))]
    scratch += [dma((n_cut, n_head - 1)), dma((n_cut, n_head - 1))]

    def body(*refs):
        fused_kernel(n_seq, n_head, head_local, tokens, *refs[:16], cuts, *refs[16:])

    vmem = pl.BlockSpec(memory_space=pltpu.VMEM)
    anywhere = pl.BlockSpec(memory_space=pl.ANY)
    grad_rows, grad_latent = pl.pallas_call(
        body,
        out_shape=(
            jax.ShapeDtypeStruct((head_local, width, tokens), bf),
            jax.ShapeDtypeStruct((width, tokens), f32),
        ),
        in_specs=[anywhere, anywhere, vmem, vmem],
        out_specs=(anywhere, vmem),
        scratch_shapes=scratch,
        compiler_params=pltpu.CompilerParams(
            collective_id=0, has_side_effects=True, vmem_limit_bytes=60 * 1024 * 1024
        ),
    )(
        queries.transpose(1, 2, 0),
        grad_out,
        latent_kv.T,
        first,
    )
    return grad_rows.transpose(2, 0, 1), grad_latent.T


def solution(mesh):
    in_specs = (P("seq", "head", None), P("seq", None), P("seq", "head", None), P("seq"))
    out_specs = (P("seq", "head", None), P("seq", None))
    n_seq, n_head = mesh.shape["seq"], mesh.shape["head"]

    def routed(queries, latent_kv, grad_out, doc_start):
        tokens, head_local, _ = queries.shape
        fits = (
            n_head > 1
            and tokens % 128 == 0
            and tokens % (16 * n_head) == 0
            and head_local % (2 * TILE_HEADS) == 0
            and n_seq >= REACH
        )
        run = partial(fused_per_device, n_seq, n_head) if fits else per_device
        return run(queries, latent_kv, grad_out, doc_start)

    return jax.shard_map(
        routed, mesh=mesh, in_specs=in_specs, out_specs=out_specs, check_vma=False
    )
```
